32 devices in a mesh: groups: 2 (over y), chan: 4 (over z), dop: 2 (over x), sub: 2 (over core).
Axes of the slice: x: 2, y: 2, z: 4, core: 2. Of those that a mesh axis runs over, the one named last changes fastest.
Arguments:
- power: bfloat16 [2, 512, 128, 1024], P(None, ('groups', 'chan', 'sub'), 'dop'), parts along dimension 1, may hold values from 0.049804688 to 20
- window: int32 [4, 2], P('groups'), parts along dimension 0, may hold values from 1 to 32, as said below
- calib_index: int32 [4, 32], P('groups', ('chan', 'sub')), parts along dimension 0, may hold values from 0 to 15
- calib_table: float32 [16], replicated, may hold values from 0.5 to 8
Outputs:
- test_ratio: float32 [2, 256, 1024], P(None, ('groups', 'dop'), ('chan', 'sub')), parts along dimension 1
The draws below stay inside these ranges and needn't reach their ends.
There are 2 independent parts, one for each index of `groups`. The reference program is written for one: setup_inputs(seed, part) draws one part's arguments, and reference() takes and returns one part's arrays. A program takes and returns all parts, laid end to end along the dimension named above; an argument that names none is the same for every part. Nothing has to cross between parts.
Inputs may be any that keep to these rules, and one draw needn't show every extreme that they name: window[c, 0] is the guard count, from 1 to 8; window[c, 1] is the reach, from 16 to 32; interval 0 has reach 32.
All inputs are finite; a program needn't handle non-finite values.
Results may differ from the reference program's by a relative error of at most 0.0003.
Values sent between devices are 32-bit elements; how exact they have to be, the bound alone decides.
A program may use at most 64 MiB of HBM per device.

```python
import math
import jax
import jax.numpy as jnp

CH = 256
DOP = 128
CPIS = 2
HALO = 32
CALIB = 32
LEVELS = 16
RANGE = 1024


def draw_window(key, part):
    guard_key = jax.random.fold_in(key, 11)
    reach_key = jax.random.fold_in(key, 23)
    guard = jax.random.randint(guard_key, (CPIS,), 1, 9)
    reach = jax.random.randint(reach_key, (CPIS,), 16, HALO + 1)
    reach = reach.at[0].set(HALO)
    return jnp.stack([guard, reach], axis=1).astype(jnp.int32)


def place_ends(result, key, least, largest):
    longest = result.shape.index(max(result.shape))
    spots = []
    for shift in (0, 1):
        where = [jax.random.randint(jax.random.fold_in(key, axis), (), 0, length) for axis, length in enumerate(result.shape)]
        where[longest] = (where[longest] + shift) % result.shape[longest]
        spots.append(tuple(where))
    return result.at[spots[0]].set(least).at[spots[1]].set(largest)


def level_of(key, dims, split, least, largest):
    def one(axis_at, shards_of):
        steps = jax.random.uniform(jax.random.fold_in(jax.random.fold_in(key, 6), axis_at), (shards_of,), jnp.float32, least / len(split), largest / len(split))
        return jnp.repeat(jnp.exp(steps), dims[axis_at] // shards_of).reshape((-1,) + (1,) * (len(dims) - axis_at - 1))

    loudness = one(*split[0])
    for cut in split[1:]:
        loudness = loudness * one(*cut)
    return loudness


def setup_inputs(seed: int = 0, part: int = 0) -> dict:
    key_list = jax.random.split(jax.random.key(seed), 5)
    part_splits = jax.random.split(jax.random.fold_in(key_list[4], part), 5)
    return {
        "power": jnp.clip(jnp.exp(math.log(20.0) - 5.9953784 * jax.random.uniform(part_splits[0], (CPIS, CH, DOP, RANGE), jnp.float32) ** level_of(part_splits[0], (CPIS, CH, DOP, RANGE), ((1, 8), (2, 2)), -0.2, 0.2)), 0.049804688, 20.0).astype(jnp.bfloat16),
        "window": draw_window(jax.random.fold_in(jax.random.fold_in(key_list[4], part), 71), part),
        "calib_index": place_ends(jax.random.randint(part_splits[2], (CPIS, RANGE // CALIB), 0, LEVELS), jax.random.fold_in(part_splits[2], 1), 0, LEVELS - 1).astype(jnp.int32),
        "calib_table": jnp.clip(jnp.exp(jax.random.uniform(key_list[3], (LEVELS,), jnp.float32, math.log(0.5), math.log(8.0))), 0.5, 8.0),
    }


def reference(power, window, calib_index, calib_table):
    integrated = jnp.sum(power, axis=1, dtype=jnp.float32)
    guard = window[:, 0]
    reach = window[:, 1]
    padded = jnp.pad(integrated, ((0, 0), (0, 0), (HALO, HALO)))
    total = jnp.zeros(integrated.shape, jnp.float32)
    for offset in range(1, HALO + 1):
        weight = ((offset > guard) & (offset <= reach)).astype(jnp.float32)[:, None, None]
        right = padded[:, :, HALO + offset:HALO + offset + RANGE]
        left = padded[:, :, HALO - offset:HALO - offset + RANGE]
        total = total + weight * (right + left)
    noise = total / (2.0 * (reach - guard).astype(jnp.float32))[:, None, None]
    levels = jnp.arange(LEVELS, dtype=jnp.int32)
    onehot = (calib_index[:, :, None] == levels[None, None, :]).astype(jnp.float32)
    block_scale = jnp.sum(onehot * calib_table[None, None, :], axis=-1)
    scale = jnp.broadcast_to(block_scale[:, :, None], (CPIS, RANGE // CALIB, CALIB)).reshape(CPIS, RANGE)
    return integrated / (scale[:, None, :] * noise)
```

```python
import functools

import jax
import jax.numpy as jnp
from jax import lax
from jax.experimental import pallas as pl
from jax.experimental.pallas import tpu as pltpu
from jax.sharding import PartitionSpec as P

HALO = 32
CALIB = 32
LANES = 128
CHUNK_ROWS = 32
MESH = pl.DeviceIdType.MESH


def split_dot(x, band):
    high = x.astype(jnp.bfloat16)
    rest = x - high.astype(jnp.float32)
    mid = rest.astype(jnp.bfloat16)
    low = (rest - mid.astype(jnp.float32)).astype(jnp.bfloat16)
    dot = functools.partial(jnp.dot, preferred_element_type=jnp.float32)
    return dot(high, band) + (dot(mid, band) + dot(low, band))


def kernel(
    chips, cores, window, index, table, power, out,
    raw, part, pair, total, inbox, strip, pack, halo,
    raw_sem, pair_send, pair_recv, z_send, z_recv, halo_send, halo_recv,
):
    chan = lax.axis_index("chan")
    sub = lax.axis_index("sub")
    me = chan * cores + sub
    strips = chips * cores
    other = 1 - sub
    intervals, channels, dops, _ = power.shape
    per = dops // CHUNK_ROWS
    chunks = intervals * per
    cells = LANES
    group = dops * HALO // LANES

    def load(k):
        c, r = k // per, (k % per) * CHUNK_ROWS
        return pltpu.make_async_copy(
            power.at[c, :, pl.ds(r, CHUNK_ROWS), :], raw.at[k], raw_sem.at[k]
        )

    for k in range(chunks):
        load(k).start()

    barrier = pltpu.get_barrier_semaphore()

    @pl.loop(1, strips)
    def _(step):
        peer = lax.rem(me + step, strips)
        pl.semaphore_signal(
            barrier, inc=1, device_id={"chan": peer // cores, "sub": lax.rem(peer, cores)},
            device_id_type=MESH,
        )

    def rows_of(k):
        return pl.ds(k * CHUNK_ROWS, CHUNK_ROWS)

    def channel_sum(k):
        @pl.loop(0, chips)
        def _(j):
            for s in range(cores):
                lanes = pl.ds(pl.multiple_of((j * cores + s) * cells, cells), cells)
                acc = [None] * 2
                for ch in range(channels):
                    x = raw[k, ch, :, lanes].astype(jnp.float32)
                    acc[ch % 2] = x if acc[ch % 2] is None else acc[ch % 2] + x
                part[s, j, rows_of(k), :] = acc[0] + acc[1]

    def to_pair(k):
        return pltpu.make_async_remote_copy(
            src_ref=part.at[other, :, rows_of(k), :],
            dst_ref=pair.at[:, rows_of(k), :],
            send_sem=pair_send.at[k],
            recv_sem=pair_recv.at[k],
            device_id={"sub": other},
            device_id_type=MESH,
        )

    def offset(step):
        return jnp.where(chan < chips // 2, chips - step, step)

    def to_owner(k, step):
        hop = offset(step)
        goal = lax.rem(chan + hop, chips)
        return pltpu.make_async_remote_copy(
            src_ref=total.at[goal, rows_of(k), :],
            dst_ref=inbox.at[hop - 1, rows_of(k), :],
            send_sem=z_send.at[hop - 1, k],
            recv_sem=z_recv.at[hop - 1, k],
            device_id={"chan": goal},
            device_id_type=MESH,
        )

    def from_pair(k):
        to_pair(k).wait_recv()
        for j in range(chips):
            total[j, rows_of(k), :] = part[sub, j, rows_of(k), :] + pair[j, rows_of(k), :]
        for step in range(1, chips):
            to_owner(k, step).start()

    lane = lax.broadcasted_iota(jnp.int32, (group, LANES), 1)

    def to_side(c, side):
        peer = me + (1 if side else -1)
        return pltpu.make_async_remote_copy(
            src_ref=pack.at[side, c],
            dst_ref=halo.at[side, c],
            send_sem=halo_send.at[side, c],
            recv_sem=halo_recv.at[side, c],
            device_id={"chan": peer // cores, "sub": lax.rem(peer, cores)},
            device_id_type=MESH,
        )

    has = (me > 0, me < strips - 1)

    def collect(c):
        for k in range(c * per, (c + 1) * per):
            for hop in range(1, chips):
                to_owner(k, hop).wait_recv()
            value = total[chan, rows_of(k), :]
            for hop in range(1, chips):
                value = value + inbox[hop - 1, rows_of(k), :]
            strip[rows_of(k), :] = value
        for side in range(2):
            packed = None
            for q in range(LANES // HALO):
                x = strip[pl.ds(c * dops + q * group, group), :]
                shift = (q * HALO + side * HALO) % LANES
                x = pltpu.roll(x, shift, 1) if shift else x
                packed = x if packed is None else jnp.where(lane // HALO == q, x, packed)
            pack[side, c] = packed

            @pl.when(has[side])
            def _():
                to_side(c, side).start()

    for k in range(chunks):
        load(k).wait()
        channel_sum(k)
        if k == 0:
            pl.semaphore_wait(barrier, strips - 1)
        to_pair(k).start()
        if k >= 1:
            from_pair(k - 1)
    from_pair(chunks - 1)

    source = lax.broadcasted_iota(jnp.int32, (2 * LANES, LANES), 0)
    target = lax.broadcasted_iota(jnp.int32, (2 * LANES, LANES), 1)
    place = jnp.where(source < LANES + LANES // 2, source, source - 2 * LANES)
    distance = jnp.abs(place - target)
    cell = lax.broadcasted_iota(jnp.int32, (1, LANES), 1)
    full_lane = lax.broadcasted_iota(jnp.int32, (dops, LANES), 1)

    bands, gains = [], []
    for c in range(intervals):
        guard, reach = window[c, 0], window[c, 1]
        bands.append(
            jnp.where((distance > guard) & (distance <= reach), 1.0, 0.0).astype(jnp.bfloat16)
        )
        scale = jnp.zeros((1, LANES), jnp.float32)
        for b in range(cells // CALIB):
            scale = jnp.where(cell // CALIB == b, table[index[c, b]], scale)
        count = jnp.full((1, LANES), 2 * (reach - guard), jnp.int32).astype(jnp.float32)
        gains.append((scale, count))

    for c in range(intervals):
        collect(c)

    for c in range(intervals):
        for side in range(2):
            @pl.when(has[1 - side])
            def _():
                to_side(c, side).wait_recv()

            @pl.when(jnp.logical_not(has[1 - side]))
            def _():
                halo[side, c] = jnp.zeros((group, LANES), jnp.float32)

        wide = []
        for side in range(2):
            pieces = []
            for q in range(LANES // HALO):
                x = halo[side, c]
                shift = (LANES - q * HALO - side * HALO) % LANES
                pieces.append(pltpu.roll(x, shift, 1) if shift else x)
            wide.append(jnp.concatenate(pieces, axis=0))
        edge = jnp.where(full_lane < LANES // 2, wide[0], wide[1])
        mine = strip[pl.ds(c * dops, dops), :]
        window_sum = split_dot(jnp.concatenate([mine, edge], axis=1), bands[c])
        scale, count = gains[c]
        noise = window_sum / count
        out[c] = mine / (scale * noise)

    for k in range(chunks):
        to_pair(k).wait_send()
        for step in range(1, chips):
            to_owner(k, step).wait_send()
    for c in range(intervals):
        for side in range(2):
            @pl.when(has[side])
            def _():
                to_side(c, side).wait_send()


def solution(mesh):
    chips, cores = mesh.shape["chan"], mesh.shape["sub"]

    def body(power, window, calib_index, calib_table):
        intervals, channels, dops, cells = power.shape
        width = cells // (chips * cores)
        rows = intervals * dops
        chunks = rows // CHUNK_ROWS
        group = dops * HALO // LANES
        f32 = jnp.float32
        return pl.pallas_call(
            functools.partial(kernel, chips, cores),
            out_shape=jax.ShapeDtypeStruct((intervals, dops, width), f32),
            in_specs=[pl.BlockSpec(memory_space=pltpu.SMEM)] * 3
            + [pl.BlockSpec(memory_space=pl.ANY)],
            out_specs=pl.BlockSpec(memory_space=pltpu.VMEM),
            scratch_shapes=[
                pltpu.VMEM((chunks, channels, CHUNK_ROWS, cells), power.dtype),
                pltpu.VMEM((cores, chips, rows, width), f32),
                pltpu.VMEM((chips, rows, width), f32),
                pltpu.VMEM((chips, rows, width), f32),
                pltpu.VMEM((chips - 1, rows, width), f32),
                pltpu.VMEM((rows, width), f32),
                pltpu.VMEM((2, intervals, group, LANES), f32),
                pltpu.VMEM((2, intervals, group, LANES), f32),
                pltpu.SemaphoreType.DMA((chunks,)),
                pltpu.SemaphoreType.DMA((chunks,)),
                pltpu.SemaphoreType.DMA((chunks,)),
                pltpu.SemaphoreType.DMA((chips - 1, chunks)),
                pltpu.SemaphoreType.DMA((chips - 1, chunks)),
                pltpu.SemaphoreType.DMA((2, intervals)),
                pltpu.SemaphoreType.DMA((2, intervals)),
            ],
            compiler_params=pltpu.CompilerParams(collective_id=0, has_side_effects=True),
        )(window, calib_index, calib_table, power)

    return jax.shard_map(
        body,
        mesh=mesh,
        in_specs=(
            P(None, ("groups", "chan", "sub"), "dop", None),
            P("groups", None),
            P("groups", ("chan", "sub")),
            P(),
        ),
        out_specs=P(None, ("groups", "dop"), ("chan", "sub")),
        check_vma=False,
    )
```

```python
import functools

import jax
import jax.numpy as jnp
from jax import lax
from jax.experimental import pallas as pl
from jax.experimental.pallas import tpu as pltpu
from jax.sharding import PartitionSpec as P

HALO = 32
CALIB = 32
LANES = 128
CHUNK_ROWS = 32
VMEM_LIMIT = 60 * 2**20
MESH = pl.DeviceIdType.MESH


def split_dot(x, band):
    high = x.astype(jnp.bfloat16)
    rest = x - high.astype(jnp.float32)
    mid = rest.astype(jnp.bfloat16)
    low = (rest - mid.astype(jnp.float32)).astype(jnp.bfloat16)
    dot = functools.partial(jnp.dot, preferred_element_type=jnp.float32)
    return dot(high, band) + (dot(mid, band) + dot(low, band))


def kernel(
    chips, cores, window_in, index_in, table_in, power, top, bottom,
    window, index, table, small_sem,
    raw, part, pair, total, inbox, strip, pack, halo,
    raw_sem, pair_send, pair_recv, z_send, z_recv, halo_send, halo_recv,
):
    chan = lax.axis_index("chan")
    sub = lax.axis_index("sub")
    me = chan * cores + sub
    strips = chips * cores
    other = 1 - sub
    intervals, channels, dops, _ = power.shape
    per = dops // CHUNK_ROWS
    chunks = intervals * per
    cells = LANES
    group = dops * HALO // LANES

    def load(k):
        c, r = k // per, (k % per) * CHUNK_ROWS
        return pltpu.make_async_copy(
            power.at[c, :, pl.ds(r, CHUNK_ROWS), :], raw.at[k], raw_sem.at[k]
        )

    for k in range(chunks):
        load(k).start()

    small = [
        pltpu.make_async_copy(source, target, small_sem.at[i])
        for i, (source, target) in enumerate(
            ((window_in, window), (index_in, index), (table_in, table))
        )
    ]
    for copy in small:
        copy.start()

    barrier = pltpu.get_barrier_semaphore()

    @pl.loop(1, strips)
    def _(step):
        peer = lax.rem(me + step, strips)
        pl.semaphore_signal(
            barrier, inc=1, device_id={"chan": peer // cores, "sub": lax.rem(peer, cores)},
            device_id_type=MESH,
        )

    def rows_of(k):
        return pl.ds(k * CHUNK_ROWS, CHUNK_ROWS)

    def channel_sum(k):
        @pl.loop(0, chips, unroll=True)
        def _(j):
            for s in range(cores):
                lanes = pl.ds(pl.multiple_of((j * cores + s) * cells, cells), cells)
                acc = [None] * 2
                for ch in range(channels):
                    x = raw[k, ch, :, lanes].astype(jnp.float32)
                    acc[ch % 2] = x if acc[ch % 2] is None else acc[ch % 2] + x
                part[s, k, j] = acc[0] + acc[1]

    def to_pair(k):
        return pltpu.make_async_remote_copy(
            src_ref=part.at[other, k],
            dst_ref=pair.at[k],
            send_sem=pair_send.at[k],
            recv_sem=pair_recv.at[k],
            device_id={"sub": other},
            device_id_type=MESH,
        )

    def offset(step):
        return jnp.where(chan < chips // 2, chips - step, step)

    def to_owner(k, step):
        hop = offset(step)
        goal = lax.rem(chan + hop, chips)
        return pltpu.make_async_remote_copy(
            src_ref=total.at[k, goal],
            dst_ref=inbox.at[hop - 1, k],
            send_sem=z_send.at[hop - 1, k],
            recv_sem=z_recv.at[hop - 1, k],
            device_id={"chan": goal},
            device_id_type=MESH,
        )

    def from_pair(k):
        to_pair(k).wait_recv()
        for j in range(chips):
            total[k, j] = part[sub, k, j] + pair[k, j]
        for step in range(1, chips):
            to_owner(k, step).start()

    lane = lax.broadcasted_iota(jnp.int32, (group, LANES), 1)

    def to_side(c, side):
        peer = me + (1 if side else -1)
        return pltpu.make_async_remote_copy(
            src_ref=pack.at[side, c],
            dst_ref=halo.at[side, c],
            send_sem=halo_send.at[side, c],
            recv_sem=halo_recv.at[side, c],
            device_id={"chan": peer // cores, "sub": lax.rem(peer, cores)},
            device_id_type=MESH,
        )

    has = (me > 0, me < strips - 1)

    def collect(c):
        for k in range(c * per, (c + 1) * per):
            for hop in range(1, chips):
                to_owner(k, hop).wait_recv()
            value = total[k, chan]
            for hop in range(1, chips):
                value = value + inbox[hop - 1, k]
            strip[rows_of(k), :] = value
        for side in range(2):
            packed = None
            for q in range(LANES // HALO):
                x = strip[pl.ds(c * dops + q * group, group), :]
                shift = (q * HALO + side * HALO) % LANES
                x = pltpu.roll(x, shift, 1) if shift else x
                packed = x if packed is None else jnp.where(lane // HALO == q, x, packed)
            pack[side, c] = packed

            @pl.when(has[side])
            def _():
                to_side(c, side).start()

    for k in range(chunks):
        load(k).wait()
        channel_sum(k)
        if k == 0:
            pl.semaphore_wait(barrier, strips - 1)
        to_pair(k).start()
        if k >= 1:
            from_pair(k - 1)
    from_pair(chunks - 1)

    source = lax.broadcasted_iota(jnp.int32, (2 * LANES, LANES), 0)
    target = lax.broadcasted_iota(jnp.int32, (2 * LANES, LANES), 1)
    place = jnp.where(source < LANES + LANES // 2, source, source - 2 * LANES)
    distance = jnp.abs(place - target)
    cell = lax.broadcasted_iota(jnp.int32, (1, LANES), 1)
    full_lane = lax.broadcasted_iota(jnp.int32, (dops, LANES), 1)

    for copy in small:
        copy.wait()
    bands, gains = [], []
    for c in range(intervals):
        guard, reach = window[c, 0], window[c, 1]
        bands.append(
            jnp.where((distance > guard) & (distance <= reach), 1.0, 0.0).astype(jnp.bfloat16)
        )
        scale = jnp.zeros((1, LANES), jnp.float32)
        for b in range(cells // CALIB):
            scale = jnp.where(cell // CALIB == b, table[index[c, b]], scale)
        count = jnp.full((1, LANES), 2 * (reach - guard), jnp.int32).astype(jnp.float32)
        gains.append((scale, count))

    for c in range(intervals):
        collect(c)

    for c in range(intervals):
        for side in range(2):
            @pl.when(has[1 - side])
            def _():
                to_side(c, side).wait_recv()

            @pl.when(jnp.logical_not(has[1 - side]))
            def _():
                halo[side, c] = jnp.zeros((group, LANES), jnp.float32)

        wide = []
        for side in range(2):
            pieces = []
            for q in range(LANES // HALO):
                x = halo[side, c]
                shift = (LANES - q * HALO - side * HALO) % LANES
                pieces.append(pltpu.roll(x, shift, 1) if shift else x)
            wide.append(jnp.concatenate(pieces, axis=0))
        edge = jnp.where(full_lane < LANES // 2, wide[0], wide[1])
        mine = strip[pl.ds(c * dops, dops), :]
        window_sum = split_dot(jnp.concatenate([mine, edge], axis=1), bands[c])
        scale, count = gains[c]
        noise = window_sum / count
        top[c] = mine
        bottom[c] = scale * noise

    for k in range(chunks):
        to_pair(k).wait_send()
        for step in range(1, chips):
            to_owner(k, step).wait_send()
    for c in range(intervals):
        for side in range(2):
            @pl.when(has[side])
            def _():
                to_side(c, side).wait_send()


def solution(mesh):
    chips, cores = mesh.shape["chan"], mesh.shape["sub"]

    def body(power, window, calib_index, calib_table):
        intervals, channels, dops, cells = power.shape
        width = cells // (chips * cores)
        rows = intervals * dops
        chunks = rows // CHUNK_ROWS
        group = dops * HALO // LANES
        f32 = jnp.float32
        top, bottom = pl.pallas_call(
            functools.partial(kernel, chips, cores),
            out_shape=[pltpu.VMEM((intervals, dops, width), f32)] * 2,
            in_specs=[pl.BlockSpec(memory_space=pltpu.HBM)] * 4,
            out_specs=[pl.BlockSpec(memory_space=pltpu.VMEM)] * 2,
            scratch_shapes=[
                pltpu.SMEM(window.shape, window.dtype),
                pltpu.SMEM(calib_index.shape, calib_index.dtype),
                pltpu.SMEM(calib_table.shape, calib_table.dtype),
                pltpu.SemaphoreType.DMA((3,)),
                pltpu.VMEM((chunks, channels, CHUNK_ROWS, cells), power.dtype),
                pltpu.VMEM((cores, chunks, chips, CHUNK_ROWS, width), f32),
                pltpu.VMEM((chunks, chips, CHUNK_ROWS, width), f32),
                pltpu.VMEM((chunks, chips, CHUNK_ROWS, width), f32),
                pltpu.VMEM((chips - 1, chunks, CHUNK_ROWS, width), f32),
                pltpu.VMEM((rows, width), f32),
                pltpu.VMEM((2, intervals, group, LANES), f32),
                pltpu.VMEM((2, intervals, group, LANES), f32),
                pltpu.SemaphoreType.DMA((chunks,)),
                pltpu.SemaphoreType.DMA((chunks,)),
                pltpu.SemaphoreType.DMA((chunks,)),
                pltpu.SemaphoreType.DMA((chips - 1, chunks)),
                pltpu.SemaphoreType.DMA((chips - 1, chunks)),
                pltpu.SemaphoreType.DMA((2, intervals)),
                pltpu.SemaphoreType.DMA((2, intervals)),
            ],
            compiler_params=pltpu.CompilerParams(
                collective_id=0, has_side_effects=True, vmem_limit_bytes=VMEM_LIMIT
            ),
        )(window, calib_index, calib_table, power)
        return top / bottom

    return jax.shard_map(
        body,
        mesh=mesh,
        in_specs=(
            P(None, ("groups", "chan", "sub"), "dop", None),
            P("groups", None),
            P("groups", ("chan", "sub")),
            P(),
        ),
        out_specs=P(None, ("groups", "dop"), ("chan", "sub")),
        check_vma=False,
    )
```
